32 devices in a mesh: section: 2 (over x), fsdp: 16 (over z, y, core).
Axes of the slice: x: 2, y: 2, z: 4, core: 2. Of those that a mesh axis runs over, the one named last changes fastest.
Arguments:
- tokens: bfloat16 [6, 512, 4096], P(None, 'fsdp'), may hold values from -6 to 6
- cotangent: bfloat16 [6, 512, 4096], P(None, 'fsdp'), may hold values from -6 to 6
- order: int32 [6], replicated, may hold values from 0 to 5, each once
- w_value: bfloat16 [2, 4096, 512], P('section', 'fsdp'), may hold values from -0.09375 to 0.09375
- w_out: bfloat16 [2, 512, 4096], P('section', None, 'fsdp'), may hold values from -0.25 to 0.25
- adapter_down: bfloat16 [2, 4096, 128], P('section', 'fsdp'), may hold values from -0.09375 to 0.09375
- adapter_up: bfloat16 [2, 128, 512], P('section', None, 'fsdp'), may hold values from -0.5 to 0.5
Outputs:
- input_grads: bfloat16 [2, 6, 512, 4096], P('section', None, 'fsdp')
- grad_down: float32 [2, 4096, 128], P('section', 'fsdp')
- grad_up: float32 [2, 128, 512], P('section', None, 'fsdp')
The draws below stay inside these ranges and needn't reach their ends.
Inputs may be any that keep to these rules, and one draw needn't show every extreme that they name: order names each microbatch 0 .. 5 exactly once.
All inputs are finite; a program needn't handle non-finite values.
Results may differ from the reference program's by a relative error of at most 0.02.
Values may be sent and summed in bfloat16 or wider, within the bound.
A program may use at most 128 MiB of HBM per device.

```python
import jax
import jax.numpy as jnp
from jax import lax

D = 4096
HV = 512
R = 128
MICRO = 6
MB = 512
SECTIONS = 2


def with_spikes(entries, own_key, source, target, blocks, factor):
    def block_of(dim):
        return (jnp.arange(entries.shape[dim]) // (entries.shape[dim] // blocks)).reshape((-1,) + (1,) * (entries.ndim - 1 - dim))

    near = jax.random.permutation(own_key, blocks)[block_of(target)]
    second = (block_of(target) + blocks // 2) % blocks
    return jnp.where((block_of(source) == near) | (block_of(source) == second), factor * entries, entries)


def level_of(own_key, dims, pieces, least, top_value):
    gain, own = 1.0, jax.random.fold_in(own_key, 6)
    for dim, blocks in pieces:
        draws = jnp.exp(jax.random.uniform(jax.random.fold_in(own, dim), (blocks,), jnp.float32, least / len(pieces), top_value / len(pieces)))
        gain = gain * jnp.repeat(draws, dims[dim] // blocks).reshape([-1 if axis == dim else 1 for axis in range(len(dims))])
    return gain


def noise(rng, extent, width, most, cuts=(), kind=jnp.bfloat16):
    gain = level_of(rng, extent, cuts, -0.22, 0.18) if cuts else 1.0
    entries = jax.random.normal(rng, extent, jnp.float32) * width * gain
    return jnp.minimum(jnp.maximum(entries, -most), most).astype(kind)


def heavy_noise(rng, shape, spread, bound, shards, heavy, held_as=jnp.bfloat16):
    array = spread * jax.random.normal(rng, shape, jnp.float32)
    if shards:
        array = array * level_of(rng, shape, shards, -0.22, 0.18)
    return jnp.clip(with_spikes(array, jax.random.fold_in(rng, 3), *heavy), -bound, bound).astype(held_as)


def setup_inputs(seed: int = 0) -> dict:
    streams_of = jax.random.split(jax.random.key(seed), 8)
    return {
        "tokens": heavy_noise(streams_of[0], (MICRO, MB, D), 1.0, 6.0, ((1, 16),), (1, 2, 16, 2.0)),
        "cotangent": heavy_noise(streams_of[1], (MICRO, MB, D), 1.0, 6.0, ((1, 16),), (1, 2, 16, 2.0)),
        "order": jax.random.permutation(streams_of[2], MICRO).astype(jnp.int32),
        "w_value": noise(streams_of[3], (SECTIONS, D, HV), D ** -0.5, 0.09375, ((0, 2), (1, 16))),
        "w_out": noise(streams_of[4], (SECTIONS, HV, D), HV ** -0.5, 0.25, ((0, 2), (2, 16))),
        "adapter_down": noise(streams_of[5], (SECTIONS, D, R), D ** -0.5, 0.09375, ((0, 2), (1, 16))),
        "adapter_up": noise(streams_of[6], (SECTIONS, R, HV), R ** -0.5, 0.5, ((0, 2), (2, 16))),
    }


epsilon = 1e-05

def layer_forward(inputs, w_val, w_proj, a_down, a_up):
    widened = inputs.astype(jnp.float32)
    inverse = lax.rsqrt(lax.optimization_barrier(jnp.mean(widened * widened, axis=-1, keepdims=True)) + epsilon)
    normed = (widened * inverse).astype(jnp.bfloat16)
    low = jnp.dot(normed, a_down, preferred_element_type=jnp.float32).astype(jnp.bfloat16)
    values = (jnp.dot(normed, w_val, preferred_element_type=jnp.float32) + jnp.dot(low, a_up, preferred_element_type=jnp.float32)).astype(jnp.bfloat16)
    outputs = (widened + jnp.dot(values, w_proj, preferred_element_type=jnp.float32)).astype(jnp.bfloat16)
    return (outputs, normed, low, inverse)

def layer_backward(inputs, inverse, upstream, w_val, w_proj, a_down, a_up):
    d_values = jnp.dot(upstream, w_proj.T, preferred_element_type=jnp.float32).astype(jnp.bfloat16)
    d_low = jnp.dot(d_values, a_up.T, preferred_element_type=jnp.float32).astype(jnp.bfloat16)
    d_normed = jnp.dot(d_values, w_val.T, preferred_element_type=jnp.float32) + jnp.dot(d_low, a_down.T, preferred_element_type=jnp.float32)
    widened = inputs.astype(jnp.float32)
    project = lax.optimization_barrier(jnp.mean(d_normed * widened, axis=-1, keepdims=True))
    d_inputs = upstream.astype(jnp.float32) + inverse * (d_normed - widened * inverse * inverse * project)
    return (d_inputs.astype(jnp.bfloat16), d_values, d_low)

def reference(tokens, cotangent, order, w_value, w_out, adapter_down, adapter_up):
    current = tokens[order].reshape(MICRO * MB, D)
    stored = []
    for section_index in range(SECTIONS):
        stored.append(current)
        current = layer_forward(current, w_value[section_index], w_out[section_index], adapter_down[section_index], adapter_up[section_index])[0]
    upstream = cotangent[order].reshape(MICRO * MB, D)
    grads_in = [None] * SECTIONS
    down_grads = [None] * SECTIONS
    up_grads = [None] * SECTIONS
    for section_index in reversed(range(SECTIONS)):
        inputs = stored[section_index]
        unused, normed, low, inverse = layer_forward(inputs, w_value[section_index], w_out[section_index], adapter_down[section_index], adapter_up[section_index])
        d_inputs, d_values, d_low = layer_backward(inputs, inverse, upstream, w_value[section_index], w_out[section_index], adapter_down[section_index], adapter_up[section_index])
        down_grads[section_index] = jnp.dot(normed.T, d_low, preferred_element_type=jnp.float32)
        up_grads[section_index] = jnp.dot(low.T, d_values, preferred_element_type=jnp.float32)
        grads_in[section_index] = d_inputs.reshape(MICRO, MB, D)
        upstream = d_inputs
    return (jnp.stack(grads_in), jnp.stack(down_grads), jnp.stack(up_grads))
```

```python
import jax
import jax.numpy as jnp
from jax import lax
from jax.sharding import PartitionSpec as P

epsilon = 1e-05


def widen_dot(left, right, dims=((1,), (0,))):
    return lax.dot_general(left, right, (dims, ((), ())), preferred_element_type=jnp.float32)


def gather_weights(w_value, w_out, adapter_down, adapter_up):
    sections = lax.axis_size("section")
    joined = jnp.concatenate([w_value[0], adapter_down[0]], axis=1)
    proj = w_out[0].T
    up = adapter_up[0].T

    def whole(block):
        full = lax.all_gather(block, ("section", "fsdp"), axis=0, tiled=True)
        return full.reshape(sections, -1, block.shape[1])

    return whole(joined), whole(proj), whole(up)


def body(tokens, cotangent, order, w_value, w_out, adapter_down, adapter_up):
    sections = lax.axis_size("section")
    position = lax.axis_index("section")
    micro, local, features = tokens.shape
    width = w_value.shape[2]
    joined, proj, up = gather_weights(w_value, w_out, adapter_down, adapter_up)

    current = tokens.reshape(micro * local, features)
    saved = []
    for layer in range(sections):
        widened = current.astype(jnp.float32)
        inverse = lax.rsqrt(jnp.mean(widened * widened, axis=-1, keepdims=True) + epsilon)
        normed = (widened * inverse).astype(jnp.bfloat16)
        last = layer == sections - 1
        if last:
            low = widen_dot(normed, joined[layer][:, width:]).astype(jnp.bfloat16)
        else:
            both = widen_dot(normed, joined[layer])
            low = both[:, width:].astype(jnp.bfloat16)
            values = (both[:, :width] + widen_dot(low, up[layer], ((1,), (1,)))).astype(jnp.bfloat16)
        saved.append((current, normed, low, inverse))
        if not last:
            current = (widened + widen_dot(values, proj[layer], ((1,), (1,)))).astype(jnp.bfloat16)

    upstream = cotangent.reshape(micro * local, features)
    grads, d_vals, d_lows = [], [], []
    for layer in reversed(range(sections)):
        inputs, normed, low, inverse = saved[layer]
        d_values = widen_dot(upstream, proj[layer]).astype(jnp.bfloat16)
        d_low = widen_dot(d_values, up[layer]).astype(jnp.bfloat16)
        d_normed = widen_dot(
            jnp.concatenate([d_values, d_low], axis=1), joined[layer], ((1,), (1,))
        )
        widened = inputs.astype(jnp.float32)
        project = jnp.mean(d_normed * widened, axis=-1, keepdims=True)
        upstream = (
            upstream.astype(jnp.float32)
            + inverse * (d_normed - widened * inverse * inverse * project)
        ).astype(jnp.bfloat16)
        grads.insert(0, upstream)
        d_vals.insert(0, d_values)
        d_lows.insert(0, d_low)

    def mine(items):
        chosen = items[0]
        for layer in range(1, sections):
            chosen = jnp.where(position == layer, items[layer], chosen)
        return chosen

    shares = lax.axis_size("fsdp")
    normed = mine([item[1] for item in saved])
    low = mine([item[2] for item in saved])
    part_down = widen_dot(normed, mine(d_lows), ((0,), (0,)))
    part_up = widen_dot(mine(d_vals), low, ((0,), (0,)))
    rank = low.shape[1]
    parts = jnp.concatenate(
        [part_down.reshape(shares, -1, rank), part_up.reshape(shares, -1, rank)], axis=1
    )
    combined = lax.psum_scatter(parts, "fsdp", scatter_dimension=0, tiled=True)[0]
    share_down = features // shares
    out = mine(grads).reshape(micro, local, features)[order]
    return (out[None], combined[:share_down][None], combined[share_down:].T[None])


def solution(mesh):
    return jax.shard_map(
        body,
        mesh=mesh,
        in_specs=(
            P(None, "fsdp", None),
            P(None, "fsdp", None),
            P(),
            P("section", "fsdp", None),
            P("section", None, "fsdp"),
            P("section", "fsdp", None),
            P("section", None, "fsdp"),
        ),
        out_specs=(
            P("section", None, "fsdp", None),
            P("section", "fsdp", None),
            P("section", None, "fsdp"),
        ),
        check_vma=False,
    )
```

```python
import functools

import jax
import jax.numpy as jnp
from jax import lax
from jax.experimental import pallas as pl
from jax.experimental.pallas import tpu as pltpu
from jax.sharding import PartitionSpec as P

epsilon = 1e-05
MESH = pl.DeviceIdType.MESH
X, Y, Z = 0, 1, 2


def plan_of(shapes):
    half0, half1 = shapes[0][0] // 2, shapes[1][0] // 2
    return (
        (0, 0, half0, (Y, Z, X)),
        (0, half0, half0, (X, Z, Y)),
        (1, 0, half1, (Z, Y, X)),
        (1, half1, half1, (Z, X, Y)),
        (2, 0, shapes[2][0], (Z, Y, X)),
    )


def spread_kernel(lines, plan, a_ref, b_ref, c_ref, a_out, b_out, c_out, own_sem, recv_sem, send_sem):
    sources, outs = (a_ref, b_ref, c_ref), (a_out, b_out, c_out)
    fsdp = lines * 4
    s, f = lax.axis_index("section"), lax.axis_index("fsdp")
    core, y, z = f % 2, (f // 2) % 2, f // 4

    def place(s_, z_, y_, c_):
        return {"section": s_, "fsdp": (z_ * 2 + y_) * 2 + c_}

    partner = place(s, z, y, 1 - core)
    across = place(1 - s, z, y, core)
    beside = place(s, z, 1 - y, core)
    above = place(s, z + 1, y, core)
    below = place(s, z - 1, y, core)

    barrier = pltpu.get_barrier_semaphore()
    for target in (partner, across, beside):
        pl.semaphore_signal(barrier, inc=1, device_id=target, device_id_type=MESH)

    @pl.when(z + 1 < lines)
    def _():
        pl.semaphore_signal(barrier, inc=1, device_id=above, device_id_type=MESH)

    @pl.when(z > 0)
    def _():
        pl.semaphore_signal(barrier, inc=1, device_id=below, device_id_type=MESH)

    ends = (z + 1 < lines).astype(jnp.int32) + (z > 0).astype(jnp.int32)
    pl.semaphore_wait(barrier, 3 + ends)

    def when(test, action):
        if test is True:
            action()
        else:
            pl.when(test)(action)

    def both(left, right):
        return right if left is True else left if right is True else left & right

    def slot_of(dx, dy, dz, c_):
        return ((s + dx) % 2) * fsdp + ((z + dz) * 2 + (y + dy) % 2) * 2 + c_

    def piece(index, slot):
        array, first, rows, _ = plan[index]
        return outs[array].at[slot, pl.ds(first, rows)]

    def sends(index, dx, dy, dz, step):
        array, first, rows, order = plan[index]
        slot = slot_of(dx, dy, dz, core)
        own = dx == 0 and dy == 0 and dz == 0
        source = sources[array].at[pl.ds(first, rows)] if own else piece(index, slot)
        gone = {X: dx != 0, Y: dy != 0, Z: dz != 0}
        result = []

        def add(way, test, target):
            copy = pltpu.make_async_remote_copy(
                src_ref=source,
                dst_ref=piece(index, slot),
                send_sem=send_sem.at[step * 5 + way],
                recv_sem=recv_sem.at[slot * len(plan) + index],
                device_id=target,
                device_id_type=MESH,
            )
            result.append((test, copy))

        for rank, dim in enumerate(order):
            if any(gone[later] for later in order[rank + 1:]):
                continue
            if dim == Z:
                if dz <= 0:
                    add(0, z + 1 < lines, above)
                if dz >= 0:
                    add(1, z > 0, below)
            elif not gone[dim]:
                add(2 + dim, True, across if dim == X else beside)
        add(4, True, partner)
        return result

    events = []
    for dx in (0, 1):
        for dy in (0, 1):
            for dz in range(1 - lines, lines):
                for index in range(len(plan)):
                    events.append((dx + dy + abs(dz), index, dx, dy, dz))
    events.sort(key=lambda event: (event[0], abs(event[4]), event[1]))
    steps = {}

    def step_of(index, dx, dy, dz):
        return steps.setdefault((index, dx, dy, dz % lines), len(steps))

    def inside(dz):
        return True if dz == 0 else (z + dz < lines) if dz > 0 else (z + dz >= 0)

    copies = []
    for array in range(3):
        copy = pltpu.make_async_copy(sources[array], outs[array].at[slot_of(0, 0, 0, core)], own_sem.at[array])
        copy.start()
        copies.append(copy)

    def arrival(index, slot):
        ref = piece(index, slot)
        sem = recv_sem.at[slot * len(plan) + index]
        pltpu.make_async_copy(ref, ref, sem).wait()

    def run(event):
        distance, index, dx, dy, dz = event
        step = step_of(index, dx, dy, dz)

        def action():
            if distance:
                arrival(index, slot_of(dx, dy, dz, core))
            for test, copy in sends(index, dx, dy, dz, step):
                when(test, copy.start)

        when(inside(dz), action)

    for event in events:
        run(event)
    for _, index, dx, dy, dz in events:
        when(inside(dz), functools.partial(arrival, index, slot_of(dx, dy, dz, 1 - core)))
    for copy in copies:
        copy.wait()
    for _, index, dx, dy, dz in events:
        for test, copy in sends(index, dx, dy, dz, step_of(index, dx, dy, dz)):
            when(both(inside(dz), test), copy.wait_send)


def spread(joined, proj, up):
    fsdp = lax.axis_size("fsdp")
    devices = fsdp * lax.axis_size("section")
    blocks = (joined, proj, up)
    plan = plan_of([block.shape for block in blocks])
    pieces = len(plan)
    return pl.pallas_call(
        functools.partial(spread_kernel, fsdp // 4, plan),
        out_shape=[jax.ShapeDtypeStruct((devices,) + b.shape, b.dtype) for b in blocks],
        in_specs=[pl.BlockSpec(memory_space=pltpu.VMEM)] * 3,
        out_specs=[pl.BlockSpec(memory_space=pl.ANY)] * 3,
        scratch_shapes=[
            pltpu.SemaphoreType.DMA((3,)),
            pltpu.SemaphoreType.DMA((devices * pieces,)),
            pltpu.SemaphoreType.DMA((fsdp * pieces * 5,)),
        ],
        compiler_params=pltpu.CompilerParams(collective_id=0, has_side_effects=True),
    )(*blocks)


def widen_dot(left, right, dims=((1,), (0,))):
    return lax.dot_general(left, right, (dims, ((), ())), preferred_element_type=jnp.float32)


def gather_weights(w_value, w_out, adapter_down, adapter_up):
    sections = lax.axis_size("section")
    joined = jnp.concatenate([w_value[0], adapter_down[0]], axis=1)
    proj = w_out[0].T
    up = adapter_up[0].T

    fsdp = lax.axis_size("fsdp")
    if sections == 2 and fsdp % 4 == 0 and fsdp <= 16:
        return tuple(
            full.reshape(sections, -1, full.shape[2]) for full in spread(joined, proj, up)
        )

    def whole(block):
        full = lax.all_gather(block, ("section", "fsdp"), axis=0, tiled=True)
        return full.reshape(sections, -1, block.shape[1])

    return whole(joined), whole(proj), whole(up)


def body(tokens, cotangent, order, w_value, w_out, adapter_down, adapter_up):
    sections = lax.axis_size("section")
    position = lax.axis_index("section")
    micro, local, features = tokens.shape
    width = w_value.shape[2]
    joined, proj, up = gather_weights(w_value, w_out, adapter_down, adapter_up)

    current = tokens.reshape(micro * local, features)
    saved = []
    for layer in range(sections):
        widened = current.astype(jnp.float32)
        inverse = lax.rsqrt(jnp.mean(widened * widened, axis=-1, keepdims=True) + epsilon)
        normed = (widened * inverse).astype(jnp.bfloat16)
        last = layer == sections - 1
        if last:
            low = widen_dot(normed, joined[layer][:, width:]).astype(jnp.bfloat16)
        else:
            both = widen_dot(normed, joined[layer])
            low = both[:, width:].astype(jnp.bfloat16)
            values = (both[:, :width] + widen_dot(low, up[layer], ((1,), (1,)))).astype(jnp.bfloat16)
        saved.append((current, normed, low, inverse))
        if not last:
            current = (widened + widen_dot(values, proj[layer], ((1,), (1,)))).astype(jnp.bfloat16)

    upstream = cotangent.reshape(micro * local, features)
    grads, d_vals, d_lows = [], [], []
    for layer in reversed(range(sections)):
        inputs, normed, low, inverse = saved[layer]
        d_values = widen_dot(upstream, proj[layer]).astype(jnp.bfloat16)
        d_low = widen_dot(d_values, up[layer]).astype(jnp.bfloat16)
        d_normed = widen_dot(
            jnp.concatenate([d_values, d_low], axis=1), joined[layer], ((1,), (1,))
        )
        widened = inputs.astype(jnp.float32)
        project = jnp.mean(d_normed * widened, axis=-1, keepdims=True)
        upstream = (
            upstream.astype(jnp.float32)
            + inverse * (d_normed - widened * inverse * inverse * project)
        ).astype(jnp.bfloat16)
        grads.insert(0, upstream)
        d_vals.insert(0, d_values)
        d_lows.insert(0, d_low)

    def mine(items):
        chosen = items[0]
        for layer in range(1, sections):
            chosen = jnp.where(position == layer, items[layer], chosen)
        return chosen

    shares = lax.axis_size("fsdp")
    normed = mine([item[1] for item in saved])
    low = mine([item[2] for item in saved])
    part_down = widen_dot(normed, mine(d_lows), ((0,), (0,)))
    part_up = widen_dot(mine(d_vals), low, ((0,), (0,)))
    rank = low.shape[1]
    parts = jnp.concatenate(
        [part_down.reshape(shares, -1, rank), part_up.reshape(shares, -1, rank)], axis=1
    )
    combined = lax.psum_scatter(parts, "fsdp", scatter_dimension=0, tiled=True)[0]
    share_down = features // shares
    out = mine(grads).reshape(micro, local, features)[order]
    return (out[None], combined[:share_down][None], combined[share_down:].T[None])


def solution(mesh):
    return jax.shard_map(
        body,
        mesh=mesh,
        in_specs=(
            P(None, "fsdp", None),
            P(None, "fsdp", None),
            P(),
            P("section", "fsdp", None),
            P("section", None, "fsdp"),
            P("section", "fsdp", None),
            P("section", None, "fsdp"),
        ),
        out_specs=(
            P("section", None, "fsdp", None),
            P("section", "fsdp", None),
            P("section", None, "fsdp"),
        ),
        check_vma=False,
    )
```

```python
import functools

import jax
import jax.numpy as jnp
from jax import lax
from jax.experimental import pallas as pl
from jax.experimental.pallas import tpu as pltpu
from jax.sharding import PartitionSpec as P

epsilon = 1e-05
MESH = pl.DeviceIdType.MESH
X, Y, Z = 0, 1, 2


def plan_of(shapes):
    half0, half1 = shapes[0][0] // 2, shapes[1][0] // 2
    return (
        (0, 0, half0, (Y, Z, X)),
        (0, half0, half0, (X, Z, Y)),
        (1, 0, half1, (Z, Y, X)),
        (1, half1, half1, (Z, X, Y)),
        (2, 0, shapes[2][0], (Z, Y, X)),
    )


def spread_kernel(lines, plan, a_ref, b_ref, c_ref, a_out, b_out, c_out, own_sem, recv_sem, send_sem):
    sources, outs = (a_ref, b_ref, c_ref), (a_out, b_out, c_out)
    fsdp = lines * 4
    s, f = lax.axis_index("section"), lax.axis_index("fsdp")
    core, y, z = f % 2, (f // 2) % 2, f // 4

    def place(s_, z_, y_, c_):
        return {"section": s_, "fsdp": (z_ * 2 + y_) * 2 + c_}

    partner = place(s, z, y, 1 - core)
    across = place(1 - s, z, y, core)
    beside = place(s, z, 1 - y, core)
    above = place(s, z + 1, y, core)
    below = place(s, z - 1, y, core)

    barrier = pltpu.get_barrier_semaphore()
    for target in (partner, across, beside):
        pl.semaphore_signal(barrier, inc=1, device_id=target, device_id_type=MESH)

    @pl.when(z + 1 < lines)
    def _():
        pl.semaphore_signal(barrier, inc=1, device_id=above, device_id_type=MESH)

    @pl.when(z > 0)
    def _():
        pl.semaphore_signal(barrier, inc=1, device_id=below, device_id_type=MESH)

    ends = (z + 1 < lines).astype(jnp.int32) + (z > 0).astype(jnp.int32)
    pl.semaphore_wait(barrier, 3 + ends)

    def when(test, action):
        if test is True:
            action()
        else:
            pl.when(test)(action)

    def both(left, right):
        return right if left is True else left if right is True else left & right

    def slot_of(dx, dy, dz, c_):
        return ((s + dx) % 2) * fsdp + ((z + dz) * 2 + (y + dy) % 2) * 2 + c_

    def piece(index, slot):
        array, first, rows, _ = plan[index]
        return outs[array].at[slot, pl.ds(first, rows)]

    def sends(index, dx, dy, dz, step):
        array, first, rows, order = plan[index]
        slot = slot_of(dx, dy, dz, core)
        own = dx == 0 and dy == 0 and dz == 0
        source = sources[array].at[pl.ds(first, rows)] if own else piece(index, slot)
        gone = {X: dx != 0, Y: dy != 0, Z: dz != 0}
        result = []

        def add(way, test, target):
            copy = pltpu.make_async_remote_copy(
                src_ref=source,
                dst_ref=piece(index, slot),
                send_sem=send_sem.at[step * 5 + way],
                recv_sem=recv_sem.at[slot * len(plan) + index],
                device_id=target,
                device_id_type=MESH,
            )
            result.append((test, copy))

        for rank, dim in enumerate(order):
            if any(gone[later] for later in order[rank + 1:]):
                continue
            if dim == Z:
                if dz <= 0:
                    add(0, z + 1 < lines, above)
                if dz >= 0:
                    add(1, z > 0, below)
            elif not gone[dim]:
                add(2 + dim, True, across if dim == X else beside)
        add(4, True, partner)
        return result

    events = []
    for dx in (0, 1):
        for dy in (0, 1):
            for dz in range(1 - lines, lines):
                for index in range(len(plan)):
                    events.append((dx + dy + abs(dz), index, dx, dy, dz))
    events.sort(key=lambda event: (event[0], abs(event[4]), event[1]))
    steps = {}

    def step_of(index, dx, dy, dz):
        return steps.setdefault((index, dx, dy, dz % lines), len(steps))

    def inside(dz):
        return True if dz == 0 else (z + dz < lines) if dz > 0 else (z + dz >= 0)

    copies = []
    for array in range(3):
        copy = pltpu.make_async_copy(sources[array], outs[array].at[slot_of(0, 0, 0, core)], own_sem.at[array])
        copy.start()
        copies.append(copy)

    def arrival(index, slot):
        ref = piece(index, slot)
        sem = recv_sem.at[slot * len(plan) + index]
        pltpu.make_async_copy(ref, ref, sem).wait()

    def run(event):
        distance, index, dx, dy, dz = event
        step = step_of(index, dx, dy, dz)

        def action():
            if distance:
                arrival(index, slot_of(dx, dy, dz, core))
            for test, copy in sends(index, dx, dy, dz, step):
                when(test, copy.start)

        when(inside(dz), action)

    for event in events:
        run(event)
    for _, index, dx, dy, dz in events:
        when(inside(dz), functools.partial(arrival, index, slot_of(dx, dy, dz, 1 - core)))
    for copy in copies:
        copy.wait()
    for _, index, dx, dy, dz in events:
        for test, copy in sends(index, dx, dy, dz, step_of(index, dx, dy, dz)):
            when(both(inside(dz), test), copy.wait_send)


def spread(joined, proj, up):
    fsdp = lax.axis_size("fsdp")
    devices = fsdp * lax.axis_size("section")
    blocks = (joined, proj, up)
    plan = plan_of([block.shape for block in blocks])
    pieces = len(plan)
    return pl.pallas_call(
        functools.partial(spread_kernel, fsdp // 4, plan),
        out_shape=[jax.ShapeDtypeStruct((devices,) + b.shape, b.dtype) for b in blocks],
        in_specs=[pl.BlockSpec(memory_space=pltpu.VMEM)] * 3,
        out_specs=[pl.BlockSpec(memory_space=pl.ANY)] * 3,
        scratch_shapes=[
            pltpu.SemaphoreType.DMA((3,)),
            pltpu.SemaphoreType.DMA((devices * pieces,)),
            pltpu.SemaphoreType.DMA((fsdp * pieces * 5,)),
        ],
        compiler_params=pltpu.CompilerParams(collective_id=0, has_side_effects=True),
    )(*blocks)


def settle_kernel(parts_ref, down_ref, up_ref, near, mine, far, near_send, near_recv, far_send, far_recv):
    chips = parts_ref.shape[0]
    f = lax.axis_index("fsdp")
    core, chip = f % 2, f // 2
    barrier = pltpu.get_barrier_semaphore()
    pl.semaphore_signal(barrier, inc=1, device_id={"fsdp": chip * 2 + 1 - core}, device_id_type=MESH)
    for step in range(1, chips):
        other = (chip + step) % chips
        pl.semaphore_signal(barrier, inc=1, device_id={"fsdp": other * 2 + core}, device_id_type=MESH)
    pl.semaphore_wait(barrier, chips)

    handed, passed = [], []
    for step in range(chips):
        other = (chip + 1 + step) % chips
        copy = pltpu.make_async_remote_copy(
            src_ref=parts_ref.at[other, 1 - core],
            dst_ref=near.at[step],
            send_sem=near_send.at[step],
            recv_sem=near_recv.at[step],
            device_id={"fsdp": chip * 2 + 1 - core},
            device_id_type=MESH,
        )
        copy.start()
        handed.append(copy)
    for step in range(chips - 1):
        other = (chip + 1 + step) % chips
        handed[step].wait_recv()
        mine[step] = (
            parts_ref[other, core].astype(jnp.float32) + near[step].astype(jnp.float32)
        ).astype(mine.dtype)
        copy = pltpu.make_async_remote_copy(
            src_ref=mine.at[step],
            dst_ref=far.at[step],
            send_sem=far_send.at[step],
            recv_sem=far_recv.at[step],
            device_id={"fsdp": other * 2 + core},
            device_id_type=MESH,
        )
        passed.append(copy)
        if step:
            passed[step - 1].start()
    handed[-1].wait_recv()
    total = parts_ref[chip, core].astype(jnp.float32) + near[chips - 1].astype(jnp.float32)
    passed[-1].start()
    for step in range(chips - 1):
        passed[step].wait_recv()
        total = total + far[step].astype(jnp.float32)
    split = down_ref.shape[0]
    down_ref[...] = total[:split]
    up_ref[...] = total[split:]
    for copy in handed + passed:
        copy.wait_send()


def settle(parts, split):
    chips, _, rows, rank = parts.shape
    buffer = pltpu.VMEM((chips, rows, rank), parts.dtype)
    return pl.pallas_call(
        settle_kernel,
        out_shape=[
            jax.ShapeDtypeStruct((split, rank), jnp.float32),
            jax.ShapeDtypeStruct((rows - split, rank), jnp.float32),
        ],
        in_specs=[pl.BlockSpec(memory_space=pltpu.VMEM)],
        out_specs=[pl.BlockSpec(memory_space=pltpu.VMEM)] * 2,
        scratch_shapes=[buffer, buffer, buffer] + [pltpu.SemaphoreType.DMA((chips,))] * 4,
        compiler_params=pltpu.CompilerParams(collective_id=1, has_side_effects=True),
    )(parts)


def widen_dot(left, right, dims=((1,), (0,))):
    return lax.dot_general(left, right, (dims, ((), ())), preferred_element_type=jnp.float32)


def custom_route():
    fsdp = lax.axis_size("fsdp")
    return lax.axis_size("section") == 2 and fsdp % 4 == 0 and fsdp <= 16


def gather_weights(w_value, w_out, adapter_down, adapter_up):
    sections = lax.axis_size("section")
    joined = jnp.concatenate([w_value[0], adapter_down[0]], axis=1)
    proj = w_out[0].T
    up = adapter_up[0].T

    if custom_route():
        return tuple(
            full.reshape(sections, -1, full.shape[2]) for full in spread(joined, proj, up)
        )

    def whole(block):
        full = lax.all_gather(block, ("section", "fsdp"), axis=0, tiled=True)
        return full.reshape(sections, -1, block.shape[1])

    return whole(joined), whole(proj), whole(up)


def body(tokens, cotangent, order, w_value, w_out, adapter_down, adapter_up):
    sections = lax.axis_size("section")
    position = lax.axis_index("section")
    micro, local, features = tokens.shape
    width = w_value.shape[2]
    joined, proj, up = gather_weights(w_value, w_out, adapter_down, adapter_up)

    current = tokens.reshape(micro * local, features)
    saved = []
    for layer in range(sections):
        widened = current.astype(jnp.float32)
        inverse = lax.rsqrt(jnp.mean(widened * widened, axis=-1, keepdims=True) + epsilon)
        normed = (widened * inverse).astype(jnp.bfloat16)
        last = layer == sections - 1
        if last:
            low = widen_dot(normed, joined[layer][:, width:]).astype(jnp.bfloat16)
        else:
            both = widen_dot(normed, joined[layer])
            low = both[:, width:].astype(jnp.bfloat16)
            values = (both[:, :width] + widen_dot(low, up[layer], ((1,), (1,)))).astype(jnp.bfloat16)
        saved.append((current, normed, low, inverse))
        if not last:
            current = (widened + widen_dot(values, proj[layer], ((1,), (1,)))).astype(jnp.bfloat16)

    upstream = cotangent.reshape(micro * local, features)
    grads, d_vals, d_lows = [], [], []
    for layer in reversed(range(sections)):
        inputs, normed, low, inverse = saved[layer]
        d_values = widen_dot(upstream, proj[layer]).astype(jnp.bfloat16)
        d_low = widen_dot(d_values, up[layer]).astype(jnp.bfloat16)
        d_normed = widen_dot(
            jnp.concatenate([d_values, d_low], axis=1), joined[layer], ((1,), (1,))
        )
        widened = inputs.astype(jnp.float32)
        project = jnp.mean(d_normed * widened, axis=-1, keepdims=True)
        upstream = (
            upstream.astype(jnp.float32)
            + inverse * (d_normed - widened * inverse * inverse * project)
        ).astype(jnp.bfloat16)
        grads.insert(0, upstream)
        d_vals.insert(0, d_values)
        d_lows.insert(0, d_low)

    def mine(items):
        chosen = items[0]
        for layer in range(1, sections):
            chosen = jnp.where(position == layer, items[layer], chosen)
        return chosen

    shares = lax.axis_size("fsdp")
    normed = mine([item[1] for item in saved])
    low = mine([item[2] for item in saved])
    part_down = widen_dot(normed, mine(d_lows), ((0,), (0,)))
    part_up = widen_dot(mine(d_vals), low, ((0,), (0,)))
    rank = low.shape[1]
    parts = jnp.concatenate(
        [part_down.reshape(shares, -1, rank), part_up.reshape(shares, -1, rank)], axis=1
    )
    share_down = features // shares
    if custom_route():
        split = parts.astype(jnp.bfloat16).reshape(shares // 2, 2, *parts.shape[1:])
        grad_down, grad_up = settle(split, share_down)
    else:
        combined = lax.psum_scatter(parts, "fsdp", scatter_dimension=0, tiled=True)[0]
        grad_down, grad_up = combined[:share_down], combined[share_down:]
    out = mine(grads).reshape(micro, local, features)[order]
    return (out[None], grad_down[None], grad_up.T[None])


def solution(mesh):
    return jax.shard_map(
        body,
        mesh=mesh,
        in_specs=(
            P(None, "fsdp", None),
            P(None, "fsdp", None),
            P(),
            P("section", "fsdp", None),
            P("section", None, "fsdp"),
            P("section", "fsdp", None),
            P("section", None, "fsdp"),
        ),
        out_specs=(
            P("section", None, "fsdp", None),
            P("section", "fsdp", None),
            P("section", None, "fsdp"),
        ),
        check_vma=False,
    )
```

```python
import functools

import jax
import jax.numpy as jnp
from jax import lax
from jax.experimental import pallas as pl
from jax.experimental.pallas import tpu as pltpu
from jax.sharding import PartitionSpec as P

epsilon = 1e-05
MESH = pl.DeviceIdType.MESH
X, Y, Z = 0, 1, 2


def plan_of(shapes):
    half0, half1 = shapes[0][0] // 2, shapes[1][0] // 2
    return (
        (0, 0, half0, (Y, Z, X)),
        (0, half0, half0, (X, Z, Y)),
        (1, 0, half1, (Z, Y, X)),
        (1, half1, half1, (Z, X, Y)),
        (2, 0, shapes[2][0], (Z, Y, X)),
    )


def spread_kernel(lines, plan, a_ref, b_ref, c_ref, a_out, b_out, c_out, own_sem, recv_sem, send_sem):
    sources, outs = (a_ref, b_ref, c_ref), (a_out, b_out, c_out)
    fsdp = lines * 4
    s, f = lax.axis_index("section"), lax.axis_index("fsdp")
    core, y, z = f % 2, (f // 2) % 2, f // 4

    def place(s_, z_, y_, c_):
        return {"section": s_, "fsdp": (z_ * 2 + y_) * 2 + c_}

    partner = place(s, z, y, 1 - core)
    across = place(1 - s, z, y, core)
    beside = place(s, z, 1 - y, core)
    above = place(s, z + 1, y, core)
    below = place(s, z - 1, y, core)

    barrier = pltpu.get_barrier_semaphore()
    for target in (partner, across, beside):
        pl.semaphore_signal(barrier, inc=1, device_id=target, device_id_type=MESH)

    @pl.when(z + 1 < lines)
    def _():
        pl.semaphore_signal(barrier, inc=1, device_id=above, device_id_type=MESH)

    @pl.when(z > 0)
    def _():
        pl.semaphore_signal(barrier, inc=1, device_id=below, device_id_type=MESH)

    ends = (z + 1 < lines).astype(jnp.int32) + (z > 0).astype(jnp.int32)
    pl.semaphore_wait(barrier, 3 + ends)

    def when(test, action):
        if test is True:
            action()
        else:
            pl.when(test)(action)

    def both(left, right):
        return right if left is True else left if right is True else left & right

    def slot_of(dx, dy, dz, c_):
        return ((s + dx) % 2) * fsdp + ((z + dz) * 2 + (y + dy) % 2) * 2 + c_

    def piece(index, slot):
        array, first, rows, _ = plan[index]
        return outs[array].at[slot, pl.ds(first, rows)]

    def sends(index, dx, dy, dz, step):
        array, first, rows, order = plan[index]
        slot = slot_of(dx, dy, dz, core)
        own = dx == 0 and dy == 0 and dz == 0
        source = sources[array].at[pl.ds(first, rows)] if own else piece(index, slot)
        gone = {X: dx != 0, Y: dy != 0, Z: dz != 0}
        result = []

        def add(way, test, target):
            copy = pltpu.make_async_remote_copy(
                src_ref=source,
                dst_ref=piece(index, slot),
                send_sem=send_sem.at[step * 5 + way],
                recv_sem=recv_sem.at[slot * len(plan) + index],
                device_id=target,
                device_id_type=MESH,
            )
            result.append((test, copy))

        for rank, dim in enumerate(order):
            if any(gone[later] for later in order[rank + 1:]):
                continue
            if dim == Z:
                if dz <= 0:
                    add(0, z + 1 < lines, above)
                if dz >= 0:
                    add(1, z > 0, below)
            elif not gone[dim]:
                add(2 + dim, True, across if dim == X else beside)
        add(4, True, partner)
        return result

    events = []
    for dx in (0, 1):
        for dy in (0, 1):
            for dz in range(1 - lines, lines):
                for index in range(len(plan)):
                    events.append((dx + dy + abs(dz), index, dx, dy, dz))
    events.sort(key=lambda event: (event[0], abs(event[4]), event[1]))
    steps = {}

    def step_of(index, dx, dy, dz):
        return steps.setdefault((index, dx, dy, dz % lines), len(steps))

    def inside(dz):
        return True if dz == 0 else (z + dz < lines) if dz > 0 else (z + dz >= 0)

    copies = []
    for array in range(3):
        copy = pltpu.make_async_copy(sources[array], outs[array].at[slot_of(0, 0, 0, core)], own_sem.at[array])
        copy.start()
        copies.append(copy)

    def arrival(index, slot):
        ref = piece(index, slot)
        sem = recv_sem.at[slot * len(plan) + index]
        pltpu.make_async_copy(ref, ref, sem).wait()

    def run(event):
        distance, index, dx, dy, dz = event
        step = step_of(index, dx, dy, dz)

        def action():
            if distance:
                arrival(index, slot_of(dx, dy, dz, core))
            for test, copy in sends(index, dx, dy, dz, step):
                when(test, copy.start)

        when(inside(dz), action)

    for event in events:
        run(event)
    for _, index, dx, dy, dz in events:
        when(inside(dz), functools.partial(arrival, index, slot_of(dx, dy, dz, 1 - core)))
    for copy in copies:
        copy.wait()
    for _, index, dx, dy, dz in events:
        for test, copy in sends(index, dx, dy, dz, step_of(index, dx, dy, dz)):
            when(both(inside(dz), test), copy.wait_send)


def spread(joined, proj, up):
    fsdp = lax.axis_size("fsdp")
    devices = fsdp * lax.axis_size("section")
    blocks = (joined, proj, up)
    plan = plan_of([block.shape for block in blocks])
    pieces = len(plan)
    return pl.pallas_call(
        functools.partial(spread_kernel, fsdp // 4, plan),
        out_shape=[jax.ShapeDtypeStruct((devices,) + b.shape, b.dtype) for b in blocks],
        in_specs=[pl.BlockSpec(memory_space=pltpu.VMEM)] * 3,
        out_specs=[pl.BlockSpec(memory_space=pl.ANY)] * 3,
        scratch_shapes=[
            pltpu.SemaphoreType.DMA((3,)),
            pltpu.SemaphoreType.DMA((devices * pieces,)),
            pltpu.SemaphoreType.DMA((fsdp * pieces * 5,)),
        ],
        compiler_params=pltpu.CompilerParams(collective_id=0, has_side_effects=True),
    )(*blocks)


def settle_kernel(parts_ref, down_ref, up_ref, near, mine, far, near_send, near_recv, far_send, far_recv):
    chips = parts_ref.shape[0]
    f = lax.axis_index("fsdp")
    core, chip = f % 2, f // 2
    barrier = pltpu.get_barrier_semaphore()
    pl.semaphore_signal(barrier, inc=1, device_id={"fsdp": chip * 2 + 1 - core}, device_id_type=MESH)
    for step in range(1, chips):
        other = (chip + step) % chips
        pl.semaphore_signal(barrier, inc=1, device_id={"fsdp": other * 2 + core}, device_id_type=MESH)
    pl.semaphore_wait(barrier, chips)

    handed, passed = [], []
    for step in range(chips):
        other = (chip + 1 + step) % chips
        copy = pltpu.make_async_remote_copy(
            src_ref=parts_ref.at[other, 1 - core],
            dst_ref=near.at[step],
            send_sem=near_send.at[step],
            recv_sem=near_recv.at[step],
            device_id={"fsdp": chip * 2 + 1 - core},
            device_id_type=MESH,
        )
        copy.start()
        handed.append(copy)
    for step in range(chips - 1):
        other = (chip + 1 + step) % chips
        handed[step].wait_recv()
        mine[step] = (
            parts_ref[other, core].astype(jnp.float32) + near[step].astype(jnp.float32)
        ).astype(mine.dtype)
        copy = pltpu.make_async_remote_copy(
            src_ref=mine.at[step],
            dst_ref=far.at[step],
            send_sem=far_send.at[step],
            recv_sem=far_recv.at[step],
            device_id={"fsdp": other * 2 + core},
            device_id_type=MESH,
        )
        passed.append(copy)
        if step:
            passed[step - 1].start()
    handed[-1].wait_recv()
    total = parts_ref[chip, core].astype(jnp.float32) + near[chips - 1].astype(jnp.float32)
    passed[-1].start()
    for step in range(chips - 1):
        passed[step].wait_recv()
        total = total + far[step].astype(jnp.float32)
    split = down_ref.shape[0]
    down_ref[...] = total[:split]
    up_ref[...] = total[split:]
    for copy in handed + passed:
        copy.wait_send()


def settle(parts, split):
    chips, _, rows, rank = parts.shape
    buffer = pltpu.VMEM((chips, rows, rank), parts.dtype)
    return pl.pallas_call(
        settle_kernel,
        out_shape=[
            jax.ShapeDtypeStruct((split, rank), jnp.float32),
            jax.ShapeDtypeStruct((rows - split, rank), jnp.float32),
        ],
        in_specs=[pl.BlockSpec(memory_space=pltpu.VMEM)],
        out_specs=[pl.BlockSpec(memory_space=pltpu.VMEM)] * 2,
        scratch_shapes=[buffer, buffer, buffer] + [pltpu.SemaphoreType.DMA((chips,))] * 4,
        compiler_params=pltpu.CompilerParams(collective_id=1, has_side_effects=True),
    )(parts)


def widen_dot(left, right, dims=((1,), (0,))):
    return lax.dot_general(left, right, (dims, ((), ())), preferred_element_type=jnp.float32)


def layers_kernel(
    sections, width, order_ref, tok_ref, cot_ref, wa_any, wo_any, up_any, out_ref, parts_ref,
    wa, wo, up, states, normed, low, cats, wide, flow, acc, sems,
):
    rows, features = tok_ref.shape
    micro = out_ref.shape[0]
    step = width
    steps = features // step
    position = lax.axis_index("section")
    bf16, f32 = jnp.bfloat16, jnp.float32
    pending = {}
    for layer in range(sections):
        for kind, (source, target) in enumerate(((wa_any, wa), (up_any, up), (wo_any, wo))):
            copy = pltpu.make_async_copy(
                source.at[layer], target.at[layer], sems.at[layer * 3 + kind]
            )
            copy.start()
            pending[layer, kind] = copy

    def ready(layer, kind):
        if (layer, kind) in pending:
            pending.pop((layer, kind)).wait()

    def span(index):
        return pl.ds(pl.multiple_of(index * step, step), step)

    def loop(action, start):
        return lax.fori_loop(0, steps, action, start)

    zero = jnp.zeros((rows, 1), f32)

    def state(layer):
        return tok_ref if layer == 0 else states.at[layer - 1]

    def squares(index, total):
        piece = tok_ref[:, span(index)].astype(f32)
        return total + jnp.sum(piece * piece, axis=1, keepdims=True)

    total = loop(squares, zero)
    inverses = []
    for layer in range(sections):
        last = layer == sections - 1
        inverse = lax.rsqrt(total / features + epsilon)
        inverses.append(inverse)
        ready(layer, 0)
        start = width if last else 0
        acc[...] = jnp.zeros_like(acc)

        def project(index, carry, layer=layer, inverse=inverse, start=start):
            piece = (state(layer)[:, span(index)].astype(f32) * inverse).astype(bf16)
            normed[layer, :, span(index)] = piece
            acc[:, start:] += widen_dot(piece, wa[layer, span(index), start:])
            return carry

        loop(project, 0)
        low[layer] = acc[:, width:].astype(bf16)
        ready(layer, 1)
        ready(layer, 2)
        if not last:
            values = (acc[:, :width] + widen_dot(low[layer], up[layer], ((1,), (1,)))).astype(bf16)
            cats[layer, :, :width] = values

            def widen(index, carry, layer=layer):
                added = widen_dot(cats[layer, :, :width], wo[layer, span(index), :], ((1,), (1,)))
                piece = (state(layer)[:, span(index)].astype(f32) + added).astype(bf16)
                states[layer, :, span(index)] = piece
                back = piece.astype(f32)
                return carry + jnp.sum(back * back, axis=1, keepdims=True)

            total = loop(widen, zero)

    def backward(layer):
        upstream = cot_ref if layer == sections - 1 else flow.at[layer + 1]
        inverse = inverses[layer]
        acc[:, :width] = jnp.zeros((rows, width), f32)

        def narrow(index, carry):
            acc[:, :width] += widen_dot(upstream[:, span(index)], wo[layer, span(index), :])
            return carry

        loop(narrow, 0)
        d_values = acc[:, :width].astype(bf16)
        cats[layer, :, :width] = d_values
        cats[layer, :, width:] = widen_dot(d_values, up[layer]).astype(bf16)

        def open_up(index, carry):
            piece = widen_dot(cats[layer], wa[layer, span(index), :], ((1,), (1,)))
            wide[:, span(index)] = piece
            inputs = state(layer)[:, span(index)].astype(f32)
            return carry + jnp.sum(piece * inputs, axis=1, keepdims=True)

        mean = loop(open_up, zero) / features

        def finish(index, carry):
            inputs = state(layer)[:, span(index)].astype(f32)
            piece = upstream[:, span(index)].astype(f32) + inverse * (
                wide[:, span(index)] - inputs * inverse * inverse * mean
            )
            flow[layer, :, span(index)] = piece.astype(bf16)
            return carry

        loop(finish, 0)

    for layer in reversed(range(sections)):
        if layer == sections - 1:
            backward(layer)
        else:
            pl.when(position <= layer)(functools.partial(backward, layer))

    blocks = parts_ref.shape[0]
    share, share_up = features // blocks, width // blocks

    def contract(index, carry):
        columns = pl.ds(pl.multiple_of(index * share, share), share)
        parts_ref[index, :share, :] = widen_dot(
            normed[position, :, columns], cats[position, :, width:], ((0,), (0,))
        ).astype(bf16)
        return carry

    lax.fori_loop(0, blocks, contract, 0)
    both = widen_dot(cats[position, :, :width], low[position], ((0,), (0,))).astype(bf16)
    for index in range(blocks):
        parts_ref[index, share:, :] = both[index * share_up:(index + 1) * share_up]
    local = rows // micro
    for slot in range(micro):
        out_ref[slot] = flow[position, pl.ds(pl.multiple_of(order_ref[slot] * local, local), local), :]


def run_layers(tokens, cotangent, order, joined, proj, up):
    micro, local, features = tokens.shape
    sections, _, width = proj.shape
    rank = up.shape[2]
    rows = micro * local
    shares = lax.axis_size("fsdp")
    block = (features + width) // shares
    bf16, f32 = jnp.bfloat16, jnp.float32
    inside, outside = pl.BlockSpec(memory_space=pltpu.VMEM), pl.BlockSpec(memory_space=pl.ANY)
    return pl.pallas_call(
        functools.partial(layers_kernel, sections, width),
        out_shape=[
            jax.ShapeDtypeStruct((micro, local, features), bf16),
            jax.ShapeDtypeStruct((shares, block, rank), bf16),
        ],
        in_specs=[pl.BlockSpec(memory_space=pltpu.SMEM), inside, inside] + [outside] * 3,
        out_specs=[inside, inside],
        scratch_shapes=[
            pltpu.VMEM(joined.shape, bf16),
            pltpu.VMEM(proj.shape, bf16),
            pltpu.VMEM(up.shape, bf16),
            pltpu.VMEM((sections - 1, rows, features), bf16),
            pltpu.VMEM((sections, rows, features), bf16),
            pltpu.VMEM((sections, rows, rank), bf16),
            pltpu.VMEM((sections, rows, width + rank), bf16),
            pltpu.VMEM((rows, features), f32),
            pltpu.VMEM((sections, rows, features), bf16),
            pltpu.VMEM((rows, width + rank), f32),
            pltpu.SemaphoreType.DMA((sections * 3,)),
        ],
        compiler_params=pltpu.CompilerParams(vmem_limit_bytes=56 * 2**20),
    )(order, tokens.reshape(rows, features), cotangent.reshape(rows, features), joined, proj, up)


def custom_route():
    fsdp = lax.axis_size("fsdp")
    return lax.axis_size("section") == 2 and fsdp % 4 == 0 and fsdp <= 16


def gather_weights(w_value, w_out, adapter_down, adapter_up):
    sections = lax.axis_size("section")
    joined = jnp.concatenate([w_value[0], adapter_down[0]], axis=1)
    proj = w_out[0].T
    up = adapter_up[0].T

    if custom_route():
        return tuple(
            full.reshape(sections, -1, full.shape[2]) for full in spread(joined, proj, up)
        )

    def whole(block):
        full = lax.all_gather(block, ("section", "fsdp"), axis=0, tiled=True)
        return full.reshape(sections, -1, block.shape[1])

    return whole(joined), whole(proj), whole(up)


def body(tokens, cotangent, order, w_value, w_out, adapter_down, adapter_up):
    sections = lax.axis_size("section")
    position = lax.axis_index("section")
    micro, local, features = tokens.shape
    width = w_value.shape[2]
    joined, proj, up = gather_weights(w_value, w_out, adapter_down, adapter_up)

    if custom_route():
        out, parts = run_layers(tokens, cotangent, order, joined, proj, up)
        shares = lax.axis_size("fsdp")
        grad_down, grad_up = settle(
            parts.reshape(shares // 2, 2, *parts.shape[1:]), features // shares
        )
        return (out[None], grad_down[None], grad_up.T[None])

    current = tokens.reshape(micro * local, features)
    saved = []
    for layer in range(sections):
        widened = current.astype(jnp.float32)
        inverse = lax.rsqrt(jnp.mean(widened * widened, axis=-1, keepdims=True) + epsilon)
        normed = (widened * inverse).astype(jnp.bfloat16)
        last = layer == sections - 1
        if last:
            low = widen_dot(normed, joined[layer][:, width:]).astype(jnp.bfloat16)
        else:
            both = widen_dot(normed, joined[layer])
            low = both[:, width:].astype(jnp.bfloat16)
            values = (both[:, :width] + widen_dot(low, up[layer], ((1,), (1,)))).astype(jnp.bfloat16)
        saved.append((current, normed, low, inverse))
        if not last:
            current = (widened + widen_dot(values, proj[layer], ((1,), (1,)))).astype(jnp.bfloat16)

    upstream = cotangent.reshape(micro * local, features)
    grads, d_vals, d_lows = [], [], []
    for layer in reversed(range(sections)):
        inputs, normed, low, inverse = saved[layer]
        d_values = widen_dot(upstream, proj[layer]).astype(jnp.bfloat16)
        d_low = widen_dot(d_values, up[layer]).astype(jnp.bfloat16)
        d_normed = widen_dot(
            jnp.concatenate([d_values, d_low], axis=1), joined[layer], ((1,), (1,))
        )
        widened = inputs.astype(jnp.float32)
        project = jnp.mean(d_normed * widened, axis=-1, keepdims=True)
        upstream = (
            upstream.astype(jnp.float32)
            + inverse * (d_normed - widened * inverse * inverse * project)
        ).astype(jnp.bfloat16)
        grads.insert(0, upstream)
        d_vals.insert(0, d_values)
        d_lows.insert(0, d_low)

    def mine(items):
        chosen = items[0]
        for layer in range(1, sections):
            chosen = jnp.where(position == layer, items[layer], chosen)
        return chosen

    shares = lax.axis_size("fsdp")
    normed = mine([item[1] for item in saved])
    low = mine([item[2] for item in saved])
    part_down = widen_dot(normed, mine(d_lows), ((0,), (0,)))
    part_up = widen_dot(mine(d_vals), low, ((0,), (0,)))
    rank = low.shape[1]
    parts = jnp.concatenate(
        [part_down.reshape(shares, -1, rank), part_up.reshape(shares, -1, rank)], axis=1
    )
    share_down = features // shares
    combined = lax.psum_scatter(parts, "fsdp", scatter_dimension=0, tiled=True)[0]
    grad_down, grad_up = combined[:share_down], combined[share_down:]
    out = mine(grads).reshape(micro, local, features)[order]
    return (out[None], grad_down[None], grad_up.T[None])


def solution(mesh):
    return jax.shard_map(
        body,
        mesh=mesh,
        in_specs=(
            P(None, "fsdp", None),
            P(None, "fsdp", None),
            P(),
            P("section", "fsdp", None),
            P("section", None, "fsdp"),
            P("section", "fsdp", None),
            P("section", None, "fsdp"),
        ),
        out_specs=(
            P("section", None, "fsdp", None),
            P("section", "fsdp", None),
            P("section", None, "fsdp"),
        ),
        check_vma=False,
    )
```
